32 devices in a mesh: row: 4 (over y, x), col: 8 (over z, core).
Axes of the slice: x: 2, y: 2, z: 4, core: 2. Of those that a mesh axis runs over, the one named last changes fastest.
Arguments:
- eigenbasis: bfloat16 [16384, 16384], P('row', 'col'), may hold values from -0.046875 to 0.046875
- gradient: float32 [16384, 2048], P('row', 'col'), may hold values from -6 to 6
- moment_one: float32 [16384, 2048], P('col', 'row'), may hold values from -0.6 to 0.6
- moment_two: float32 [16384, 2048], P('col', 'row'), may hold values from 0.0001 to 0.01
Outputs:
- update: float32 [16384, 2048], P('row', 'col')
- new_one: float32 [16384, 2048], P('col', 'row')
- new_two: float32 [16384, 2048], P('col', 'row')
The draws below stay inside these ranges and needn't reach their ends.
All inputs are finite; a program needn't handle non-finite values.
Results may differ from the reference program's by a relative error of at most 0.004.
Values may be sent and summed in bfloat16 or wider, within the bound.
A program may use at most 128 MiB of HBM per device.

```python
import math
import jax
import jax.numpy as jnp

D = 16384
COLS = 2048


def spiked(entries, own_key, source, target, parts, factor):
    owner, partner = [(jnp.arange(entries.shape[position]) // (entries.shape[position] // parts)).reshape([-1 if axis == position else 1 for axis in range(entries.ndim)]) for position in (source, target)]
    chosen = jax.random.permutation(own_key, parts)[partner]
    strong = (owner == chosen) | (owner == (partner + parts // 2) % parts)
    return jnp.where(strong, factor * entries, entries)


def block_scale(own_key, extent, split, low, high):
    def one(position, blocks):
        heights = jax.random.uniform(jax.random.fold_in(jax.random.fold_in(own_key, 6), position), (blocks,), jnp.float32, low / len(split), high / len(split))
        return jnp.repeat(jnp.exp(heights), extent[position] // blocks).reshape((-1,) + (1,) * (len(extent) - position - 1))

    level = one(*split[0])
    for cut in split[1:]:
        level = level * one(*cut)
    return level


def scatter_about(own_key, dims, scale, reach, split=(), dtype=jnp.bfloat16):
    loudness = block_scale(own_key, dims, split, -0.22, 0.18) if split else 1.0
    array = jax.random.normal(own_key, dims, jnp.float32) * scale * loudness
    return jnp.minimum(jnp.maximum(array, -reach), reach).astype(dtype)


def heavy_noise(key, extent, width, limit, split, heavy, held_as=jnp.bfloat16):
    result = width * jax.random.normal(key, extent, jnp.float32)
    if split:
        result = result * block_scale(key, extent, split, -0.22, 0.18)
    return jnp.clip(spiked(result, jax.random.fold_in(key, 3), *heavy), -limit, limit).astype(held_as)


def setup_inputs(seed: int = 0) -> dict:
    key_of = jax.random.split(jax.random.key(seed), 5)
    return {
        "eigenbasis": scatter_about(key_of[0], (D, D), D ** -0.5, 0.046875, ((0, 4), (1, 8))),
        "gradient": heavy_noise(key_of[1], (D, COLS), 1.0, 6.0, ((0, 4), (1, 8)), (0, 1, 8, 2.0), jnp.float32),
        "moment_one": scatter_about(key_of[2], (D, COLS), 0.1, 0.6, ((0, 8), (1, 4)), jnp.float32),
        "moment_two": jnp.clip(jnp.exp(math.log(0.01) - 4.6051702 * jax.random.uniform(key_of[3], (D, COLS), jnp.float32) ** block_scale(key_of[3], (D, COLS), ((0, 8), (1, 4)), -0.2, 0.2)), 0.0001, 0.01),
    }


beta_one = 0.9
beta_two = 0.999
step_count = 10
epsilon = 1e-08

def reference(eigenbasis, gradient, moment_one, moment_two):
    grad_half = gradient.astype(jnp.bfloat16)
    rotated = jnp.dot(eigenbasis.T, grad_half, preferred_element_type=jnp.float32)
    new_one = beta_one * moment_one + (1.0 - beta_one) * rotated
    new_two = beta_two * moment_two + (1.0 - beta_two) * rotated * rotated
    corr_one = 1.0 - beta_one ** step_count
    corr_two = 1.0 - beta_two ** step_count
    direction = (new_one / corr_one / (jnp.sqrt(new_two / corr_two) + epsilon)).astype(jnp.bfloat16)
    update = jnp.dot(eigenbasis, direction, preferred_element_type=jnp.float32)
    return (update, new_one, new_two)
```

```python
import jax
import jax.numpy as jnp
from jax import lax
from jax.sharding import PartitionSpec as P

beta_one = 0.9
beta_two = 0.999
step_count = 10
epsilon = 1e-08


def swap(value, axis, size, offset):
    return lax.ppermute(value, axis, [(i, i ^ offset) for i in range(size)])


def local(rows, cols, eigenbasis, gradient, moment_one, moment_two):
    row, col = lax.axis_index("row"), lax.axis_index("col")
    pair = col // 2
    side = col % 2
    share = cols // rows
    width = gradient.shape[1]
    chunks = 2 if width % 256 == 0 else 1
    piece = width // chunks
    corr_one = 1.0 - beta_one**step_count
    corr_two = 1.0 - beta_two**step_count

    def pick(stack, index):
        return lax.dynamic_index_in_dim(stack, index, 0, keepdims=False)

    def columns_of(array, chunk):
        parts = [array[:, s * width + chunk * piece : s * width + (chunk + 1) * piece] for s in range(share)]
        return parts[0] if share == 1 else jnp.concatenate(parts, axis=1)

    def rotate(whole, owner):
        block = lax.dynamic_slice_in_dim(whole, owner * share, share, 0)
        block = jnp.concatenate([block[s] for s in range(share)], axis=1)
        return lax.dot_general(eigenbasis, block, (((0,), (0,)), ((), ())), preferred_element_type=jnp.float32)

    updates, ones, twos = [], [], []
    wholes = [
        lax.all_gather(
            gradient[:, k * piece : (k + 1) * piece].astype(jnp.bfloat16), "col", axis=0, tiled=False
        )
        for k in range(chunks)
    ]
    for k in range(chunks):
        whole = wholes[k]
        arrived = [
            swap(rotate(whole, row ^ s).astype(jnp.bfloat16), "row", rows, s) for s in range(rows - 1, 0, -1)
        ]
        rotated = rotate(whole, row)
        if k + 1 < chunks:
            rotated, wholes[k + 1] = lax.optimization_barrier((rotated, wholes[k + 1]))
        for part in arrived:
            rotated = rotated + part.astype(jnp.float32)
        new_one = beta_one * columns_of(moment_one, k) + (1.0 - beta_one) * rotated
        new_two = beta_two * columns_of(moment_two, k) + (1.0 - beta_two) * rotated * rotated
        direction = (new_one / corr_one / (jnp.sqrt(new_two / corr_two) + epsilon)).astype(jnp.bfloat16)
        ones.append(new_one)
        twos.append(new_two)
        stack = jnp.stack([direction] + [swap(direction, "row", rows, s) for s in range(1, rows)])

        def back(target):
            if share == 2:
                block = pick(stack, row ^ target)
            else:
                block = jnp.concatenate(
                    [pick(stack, row ^ ((2 * target + s) // share)) for s in range(2)], axis=1
                )
            return lax.dot_general(eigenbasis, block, (((1,), (0,)), ((), ())), preferred_element_type=jnp.float32)

        update = None
        for t in range(cols // 2 - 1, -1, -1):
            both = back(pair ^ t)
            keep = lax.dynamic_slice_in_dim(both, side * piece, piece, 1)
            give = lax.dynamic_slice_in_dim(both, (1 - side) * piece, piece, 1).astype(jnp.bfloat16)
            mine = keep + swap(give, "col", cols, 1).astype(jnp.float32)
            if t:
                mine = swap(mine.astype(jnp.bfloat16), "col", cols, 2 * t).astype(jnp.float32)
            update = mine if update is None else update + mine
        updates.append(update)

    def merge(pieces):
        parts = [p[:, s * piece : (s + 1) * piece] for s in range(share) for p in pieces]
        return jnp.concatenate(parts, axis=1)

    return (jnp.concatenate(updates, axis=1), merge(ones), merge(twos))


def solution(mesh):
    rows, cols = mesh.shape["row"], mesh.shape["col"]
    placed = (P("row", "col"), P("row", "col"), P("col", "row"), P("col", "row"))
    return jax.shard_map(
        lambda *arrays: local(rows, cols, *arrays),
        mesh=mesh,
        in_specs=placed,
        out_specs=(P("row", "col"), P("col", "row"), P("col", "row")),
        check_vma=False,
    )
```
